128 devices in a mesh: rows: 16 (over y, x_hi, core), grp: 8 (over x_lo, z).
Axes of the slice: x: 4 (x_hi: 2, x_lo: 2; x = x_hi * 2 + x_lo), y: 4, z: 4, core: 2. Of those that a mesh axis runs over, the one named last changes fastest.
Arguments:
- matrix: bfloat16 [98304, 16384], P(('rows', 'grp')), may hold values from -3000 to 3000, as said below
- keep_mask: int32 [16, 98304], P(None, ('rows', 'grp')), may hold values 0 or 1
Outputs:
- cosine: float32 [16384, 256], P(('rows', 'grp'))
The draws below stay inside these ranges and needn't reach their ends.
Inputs may be any that keep to these rules, and one draw needn't show every extreme that they name: `matrix`: entries are real-valued; row and column magnitudes vary.
All inputs are finite; a program needn't handle non-finite values. No bound on the sum of `keep_mask` on one device may be relied on, other than what follows from the above.
Results may differ from the reference program's by a relative error of at most 0.0003.
Values sent between devices are 32-bit elements; how exact they have to be, the bound alone decides.
No kernel may reach another device: no remote copies, remote signals or barrier semaphores. Data moves between devices by JAX's collectives and lax.ppermute only.
A program may use at most 192 MiB of HBM per device.

```python
import math
import jax
import jax.numpy as jnp
from jax import lax

COLS = 16384
BLOCK = 1024
WINDOW = 256
ROW_DEV = 768
NBLK = 16
ROWS_ALL = 98304


def draw_matrix(key, part):
    key_base, key_row, key_col = jax.random.split(jax.random.fold_in(key, 7), 3)
    position = jnp.arange(ROWS_ALL, dtype=jnp.float32) / ROWS_ALL
    row_scale = jnp.exp(position * math.log(3.0) + jax.random.uniform(key_row, (ROWS_ALL,), jnp.float32, 0.0, math.log(10.0)))
    col_scale = jnp.exp(jax.random.uniform(key_col, (COLS,), jnp.float32, 0.0, math.log(10.0)))
    base = jnp.clip(jax.random.normal(key_base, (ROWS_ALL, COLS), jnp.float32), -6.0, 6.0)
    return (base * row_scale[:, None] * col_scale[None, :]).astype(jnp.bfloat16)


def with_ends(array, key, low, top_value):
    shape = array.shape
    place = [jax.random.randint(jax.random.fold_in(key, axis), (), 0, shape[axis]) for axis in range(len(shape))]
    array = array.at[tuple(place)].set(low)
    longest = shape.index(max(shape))
    place[longest] = (place[longest] + 1) % shape[longest]
    return array.at[tuple(place)].set(top_value)


def setup_inputs(seed: int = 0) -> dict:
    arg_keys = jax.random.split(jax.random.key(seed), 3)
    matrix = draw_matrix(jax.random.fold_in(arg_keys[2], 71), 0)
    keep_mask = with_ends((jax.random.randint(arg_keys[1], (NBLK, ROWS_ALL), 0, 2) < 1).astype(jnp.int32), jax.random.fold_in(arg_keys[1], 1), 0, 1)
    return {"matrix": matrix, "keep_mask": keep_mask}


def reference(matrix, keep_mask):
    steps_count = ROWS_ALL // ROW_DEV
    blocks = matrix.reshape(steps_count, ROW_DEV, COLS)
    masks = keep_mask.reshape(NBLK, steps_count, ROW_DEV).transpose(1, 0, 2)

    def accumulate(carry, item):
        square, raw = carry
        block, block_mask = item
        square = square + lax.optimization_barrier(jnp.sum(jnp.square(block.astype(jnp.float32)), axis=0))
        gate = block_mask.T.astype(jnp.bfloat16)
        masked = (block.reshape(ROW_DEV, NBLK, BLOCK) * gate[:, :, None]).reshape(ROW_DEV, COLS)
        raw = raw + jnp.dot(masked.T, masked[:, :WINDOW], preferred_element_type=jnp.float32)
        return ((square, raw), None)
    start = (jnp.zeros((COLS,), jnp.float32), jnp.zeros((COLS, WINDOW), jnp.float32))
    (square, raw), _ = lax.scan(accumulate, start, (blocks, masks))
    inverse = 1.0 / jnp.sqrt(square + 1e-06)
    return raw * inverse[:, None] * inverse[None, :WINDOW]
```

```python
import functools

import jax
import jax.numpy as jnp
import numpy as np
from jax import lax
from jax.experimental import pallas as pl
from jax.experimental.pallas import tpu as pltpu
from jax.sharding import PartitionSpec as P

WINDOW = 256
LANE = 128
TILE = WINDOW + 8
AX = ("rows", "grp")
FLIP = (1, 3)
PARTS = ((7, 3, 5), (6, 1, 2), (4, 0))
ORDER = ((0, 1, 2), (1, 2, 0), (2, 0, 1))


def linear(x, y, z, c):
    return ((y * 2 + (x >> 1)) * 2 + c) * 8 + (x & 1) * 4 + z


def place(i):
    r, g = divmod(i, 8)
    return (((r >> 1) & 1) * 2 + (g >> 2), r >> 2, g & 3, r & 1)


def swap_cores():
    return [(i, i ^ 8) for i in range(128)]


def flips(bits, phase):
    out = []
    for i in range(128):
        k = list(place(i))
        by = FLIP[k[3] ^ phase]
        for d in range(3):
            if bits[d]:
                k[d] ^= by
        out.append((i, linear(*k)))
    return out


def target(i, c, f, s):
    k = place(i)
    return linear(*(k[d] ^ (FLIP[c] * f[d]) ^ (FLIP[1 - c] * s[d]) for d in range(3)), c)


def bits_of(s):
    return (s >> 2 & 1, s >> 1 & 1, s & 1)


def table():
    out = np.zeros((128, 2, 64), np.int32)
    for i in range(128):
        own = place(i)[3]
        for which, c in enumerate((1 - own, own)):
            n = 0
            for part, order in zip(PARTS, ORDER):
                for s in part:
                    for j in range(8):
                        f = [0, 0, 0]
                        for d, b in zip(order, bits_of(j)):
                            f[d] = b
                        out[i, which, n] = target(i, c, f, bits_of(s))
                        n += 1
    return out.reshape(128, 128)


def gram_kernel(zbit, base, fold, tab, *refs):
    blocks, (panel_t, panel, mask), rest = refs[:8], refs[8:11], refs[11:]
    if fold:
        got, keep, send, stat = rest
    else:
        out, stat = rest
    step = pl.program_id(0)

    @pl.when(step == 0)
    def _():
        p = panel[...].astype(jnp.float32)
        q = jnp.sum(p * p, axis=0, keepdims=True)
        stat[...] = jnp.concatenate([jnp.zeros((1, LANE), jnp.float32), q[:, :LANE], q[:, LANE:], jnp.zeros((5, LANE), jnp.float32)], axis=0)

    first = lax.broadcasted_iota(jnp.int32, (8, LANE), 0) == 0
    for j in range(8):
        if j & zbit:
            continue
        pair = (j, j | zbit)
        block = tab[base + step * 8 + j] // 8
        gate = (mask[pl.ds(block, 1), :] * mask[0:1, :]).astype(jnp.float32).astype(jnp.bfloat16)
        both = jnp.concatenate([blocks[k][...] for k in pair], axis=1)
        acc = jnp.dot(panel_t[...] * gate, both, preferred_element_type=jnp.float32)
        wide = both.astype(jnp.float32)
        square = jnp.sum(wide * wide, axis=0, keepdims=True)
        for n, k in enumerate(pair):
            top = acc[:, n * LANE : (n + 1) * LANE]
            low = jnp.where(first, square[:, n * LANE : (n + 1) * LANE], stat[...])
            if fold:
                ref, at = (send, k - 4) if k >= 4 else (keep, k)
                ref[0, at, :WINDOW] = top + got[0, k, :WINDOW]
                ref[0, at, WINDOW:] = low + got[0, k, WINDOW:]
            else:
                out[0, k, :WINDOW] = top
                out[0, k, WINDOW:] = low


def gram_part(tab, matrix, panel_t, mask, part, fold, got=None):
    rows = matrix.shape[0]
    count = len(PARTS[part])
    base = 64 * fold + 8 * sum(len(p) for p in PARTS[:part])
    zbit = 4 >> ORDER[part].index(2)
    whole = lambda *shape: pl.BlockSpec(shape, lambda i, t: (0,) * len(shape))
    tile = lambda n: pl.BlockSpec((1, n, TILE, LANE), lambda i, t: (i, 0, 0, 0))
    shape = lambda n: jax.ShapeDtypeStruct((count, n, TILE, LANE), jnp.float32)
    column = lambda k: pl.BlockSpec((rows, LANE), lambda i, t: (0, t[base + i * 8 + k]))
    return pl.pallas_call(
        functools.partial(gram_kernel, zbit, base, fold),
        out_shape=(shape(4), shape(4)) if fold else shape(8),
        grid_spec=pltpu.PrefetchScalarGridSpec(
            num_scalar_prefetch=1,
            grid=(count,),
            in_specs=[column(k) for k in range(8)]
            + [whole(WINDOW, rows), whole(rows, WINDOW), whole(*mask.shape)]
            + ([tile(8)] if fold else []),
            out_specs=(tile(4), tile(4)) if fold else tile(8),
            scratch_shapes=[pltpu.VMEM((8, LANE), jnp.float32)],
        ),
        compiler_params=pltpu.CompilerParams(vmem_limit_bytes=16 << 20),
        cost_estimate=pl.CostEstimate(
            flops=2 * rows * WINDOW * LANE * 8 * count,
            bytes_accessed=rows * LANE * 16 * count,
            transcendentals=0,
        ),
        name=f"gram{part}{'own' if fold else 'peer'}",
    )(tab, *([matrix] * 8), panel_t, matrix, mask, *([got] if fold else []))


def finish_kernel(*refs):
    out = refs[-1]
    total = refs[0][...]
    for r in refs[1:-1]:
        total = total + r[...]
    low = total[WINDOW:]
    inverse = 1.0 / jnp.sqrt(low + 1e-06)
    scaled = total[:WINDOW] * inverse[0:1]
    for h in range(WINDOW // LANE):
        out[:, h * LANE : (h + 1) * LANE] = scaled[h * LANE : (h + 1) * LANE].T * inverse[1 + h : 2 + h]


def shards(matrix, keep_mask):
    here = lax.axis_index("rows") * 8 + lax.axis_index("grp")
    tab = lax.dynamic_index_in_dim(jnp.asarray(table()), here, 0, keepdims=False)
    panel_t = matrix[:, :WINDOW].T
    got = []
    for p in range(3):
        peer = gram_part(tab, matrix, panel_t, keep_mask, p, 0)
        got.append(lax.ppermute(peer, AX, swap_cores()))
    keep, r1 = [], []
    unit = lambda d: tuple(int(d == k) for k in range(3))
    for p in range(3):
        k, send = gram_part(tab, matrix, panel_t, keep_mask, p, 1, got[p])
        keep.append(k)
        r1.append(lax.ppermute(send, AX, flips(unit(ORDER[p][0]), 0)))
    r2 = [lax.ppermute(keep[p][:, 2:] + r1[p][:, 2:], AX, flips(unit(ORDER[p][1]), 0)) for p in range(3)]
    r3 = [
        lax.ppermute(keep[p][:, 1:2] + r1[p][:, 1:2] + r2[p][:, 1:2], AX, flips(unit(ORDER[p][2]), 0))
        for p in range(3)
    ]
    last = []
    for p in range(3):
        for n, s in enumerate(PARTS[p]):
            mine = keep[p][n, 0] + r1[p][n, 0] + r2[p][n, 0] + r3[p][n, 0]
            last.append(lax.ppermute(mine, AX, flips(bits_of(s), 1)) if s else mine)
    return pl.pallas_call(
        finish_kernel,
        out_shape=jax.ShapeDtypeStruct((LANE, WINDOW), jnp.float32),
        name="finish",
        compiler_params=pltpu.CompilerParams(vmem_limit_bytes=8 << 20),
    )(*last)


def solution(mesh):
    in_specs = (P(AX, None), P(None, AX))
    return jax.shard_map(shards, mesh=mesh, in_specs=in_specs, out_specs=P(AX, None), check_vma=False)
```

```python
import functools

import jax
import jax.numpy as jnp
from jax import lax
from jax.experimental import pallas as pl
from jax.experimental.pallas import tpu as pltpu
from jax.sharding import PartitionSpec as P

WINDOW = 256
LANE = 128
TILE = WINDOW + 8
AX = ("rows", "grp")
FLIP = (1, 3)
PARTS = ((3, 5, 4), (0, 1, 2), (7, 6))
ORDER = ((0, 1, 2), (1, 2, 0), (2, 0, 1))
COUNT = tuple(4 * len(p) for p in PARTS)
START = (0, COUNT[0], COUNT[0] + COUNT[1])
TOTAL = sum(COUNT)
PAIRS = (
    tuple(((n, j), (n, j + 1)) for n in range(3) for j in (0, 2)),
    tuple(((n, j), (n, j + 2)) for n in range(3) for j in (0, 1)),
    tuple(((0, j), (1, j)) for j in range(4)),
)


def linear(x, y, z, c):
    return ((y * 2 + (x >> 1)) * 2 + c) * 8 + (x & 1) * 4 + z


def place(i):
    r, g = i >> 3, i & 7
    return (((r >> 1) & 1) * 2 + (g >> 2), r >> 2, g & 3, r & 1)


def swap_cores():
    return [(i, i ^ 8) for i in range(128)]


def flips(bits, phase):
    out = []
    for i in range(128):
        k = list(place(i))
        by = FLIP[k[3] ^ phase]
        for d in range(3):
            if bits[d]:
                k[d] ^= by
        out.append((i, linear(*k)))
    return out


def bits_of(s):
    return (s >> 2 & 1, s >> 1 & 1, s & 1)


def f_bits(part, half, j):
    f = [0, 0, 0]
    for d, b in zip(ORDER[part], (half, j >> 1, j & 1)):
        f[d] = b
    return f


def gram_kernel(own, half, first, here, matrix, mask, *refs):
    if first:
        *outs, panel_t, stat, gates, tiles, sems, panel, flags, panel_sems = refs
    else:
        gates = mask
        panel_t, stat, *rest = refs
        *outs, tiles, sems = rest[-5:] if half else rest[-3:]
    x, y, z, c = place(here[0])
    c = c if own else 1 - c
    near, far = 1 + 2 * c, 3 - 2 * c

    def goal(part, n, j):
        f, s = f_bits(part, half, j), bits_of(PARTS[part][n])
        by = [(0, far, near, 2)[2 * fb + sb] for fb, sb in zip(f, s)]
        return linear(x ^ by[0], y ^ by[1], z ^ by[2], c)

    def fetch(t, at):
        return pltpu.make_async_copy(matrix.at[:, pl.ds(at * LANE, LANE)], tiles.at[t], sems.at[t])

    if first:
        whole = pltpu.make_async_copy(matrix.at[:, pl.ds(0, WINDOW)], panel, panel_sems.at[0])
        whole.start()
        masks = pltpu.make_async_copy(mask, flags, panel_sems.at[1])
        masks.start()
    for p in range(3):
        for n in range(len(PARTS[p])):
            for j in range(4):
                fetch(START[p] + 4 * n + j, goal(p, n, j)).start()
    if first:
        masks.wait()
        gates[...] = (flags[...] * flags[0:1, :]).astype(jnp.float32)
        whole.wait()
        panel_t[...] = panel[...].T
        q = jnp.sum(jnp.square(panel[...].astype(jnp.float32)), axis=0, keepdims=True)
        stat[...] = jnp.concatenate([jnp.zeros((1, LANE), jnp.float32), q[:, :LANE], q[:, LANE:], jnp.zeros((5, LANE), jnp.float32)], axis=0)
    top_row = lax.broadcasted_iota(jnp.int32, (8, LANE), 0) == 0

    for p in range(3):
        for t in range(COUNT[p]):
            fetch(START[p] + t, 0).wait()
        for pair in PAIRS[p]:
            gate = gates[pl.ds(goal(p, *pair[0]) // 8, 1), :].astype(jnp.bfloat16)
            both = jnp.concatenate([tiles[START[p] + 4 * n + j] for n, j in pair], axis=1)
            acc = jnp.dot(panel_t[...] * gate, both, preferred_element_type=jnp.float32)
            square = jnp.sum(jnp.square(both.astype(jnp.float32)), axis=0, keepdims=True)
            for k, (n, j) in enumerate(pair):
                cut = slice(k * LANE, (k + 1) * LANE)
                out, at = (outs[p], n) if half else (outs[0], START[p] // 4 + n)
                out[at, j, :WINDOW] = acc[:, cut]
                out[at, j, WINDOW:] = jnp.where(top_row, square[:, cut], stat[...])


def gram(own, half, here, matrix, mask, extra=()):
    rows = matrix.shape[0]
    first = not extra
    vmem = pl.BlockSpec(memory_space=pltpu.VMEM)
    hbm = pl.BlockSpec(memory_space=pltpu.HBM)
    shapes = [jax.ShapeDtypeStruct((n, 4, TILE, LANE), jnp.float32) for n in (map(len, PARTS) if half else (TOTAL // 4,))]
    scratch = [pltpu.VMEM((TOTAL, rows, LANE), jnp.bfloat16), pltpu.SemaphoreType.DMA((TOTAL,))]
    if first:
        shapes += [jax.ShapeDtypeStruct((WINDOW, rows), jnp.bfloat16), jax.ShapeDtypeStruct((8, LANE), jnp.float32), jax.ShapeDtypeStruct(mask.shape, jnp.float32)]
        scratch += [pltpu.VMEM((rows, WINDOW), jnp.bfloat16), pltpu.VMEM(mask.shape, jnp.int32), pltpu.SemaphoreType.DMA((2,))]
    return pl.pallas_call(
        functools.partial(gram_kernel, own, half, first),
        out_shape=tuple(shapes),
        in_specs=[pl.BlockSpec(memory_space=pltpu.SMEM), hbm]
        + ([hbm] if first else [vmem] * 3 + [pl.BlockSpec(memory_space=pl.ANY)] * (len(extra) - 2)),
        out_specs=tuple(vmem for _ in shapes),
        scratch_shapes=scratch,
        compiler_params=pltpu.CompilerParams(vmem_limit_bytes=20 << 20),
        cost_estimate=pl.CostEstimate(
            flops=2 * rows * WINDOW * LANE * TOTAL, bytes_accessed=rows * LANE * 2 * TOTAL, transcendentals=0
        ),
    )(here, matrix, mask, *extra)


def finish_kernel(*refs):
    out = refs[-1]
    total = refs[0][...]
    for r in refs[1:-1]:
        total = total + r[...]
    low = total[WINDOW:]
    inverse = 1.0 / jnp.sqrt(low + 1e-06)
    scaled = total[:WINDOW] * inverse[0:1]
    for h in range(WINDOW // LANE):
        out[:, h * LANE : (h + 1) * LANE] = scaled[h * LANE : (h + 1) * LANE].T * inverse[1 + h : 2 + h]


def send(value, pairs):
    return lax.ppermute(value, AX, pairs)


def reduce_all(matrix, keep_mask):
    here = (lax.axis_index("rows") * 8 + lax.axis_index("grp")).astype(jnp.int32).reshape(1)
    unit = lambda d: tuple(int(d == k) for k in range(3))
    matrix = pltpu.with_memory_space_constraint(matrix, pltpu.HBM)
    *peer, panel_t, stat, gates = gram(0, 1, here, matrix, pltpu.with_memory_space_constraint(keep_mask, pltpu.HBM))
    got = [send(a, swap_cores()) for a in peer]
    own = gram(1, 1, here, matrix, gates, (panel_t, stat, *peer))
    first = [a + b for a, b in zip(own, got)]
    r1 = [send(first[p], flips(unit(ORDER[p][0]), 0)) for p in range(3)]
    (peer,) = gram(0, 0, here, matrix, gates, (panel_t, stat, *first))
    got = send(peer, swap_cores())
    (own,) = gram(1, 0, here, matrix, gates, (panel_t, stat, peer))

    def mine(p, n, j):
        row = slice(START[p] // 4, START[p] // 4 + len(PARTS[p])) if n is None else START[p] // 4 + n
        return own[row, j] + got[row, j] + r1[p][slice(None) if n is None else n, j]

    r2 = [send(mine(p, None, slice(2, 4)), flips(unit(ORDER[p][1]), 0)) for p in range(3)]
    r3 = [send(mine(p, None, 1) + r2[p][:, 1], flips(unit(ORDER[p][2]), 0)) for p in range(3)]
    last = []
    for p in range(3):
        for n, s in enumerate(PARTS[p]):
            tile = mine(p, n, 0) + r2[p][n, 0] + r3[p][n]
            last.append(send(tile, flips(bits_of(s), 1)) if s else tile)
    return pl.pallas_call(
        finish_kernel,
        out_shape=jax.ShapeDtypeStruct((LANE, WINDOW), jnp.float32),
        name="finish",
        compiler_params=pltpu.CompilerParams(vmem_limit_bytes=8 << 20),
    )(*last)


def solution(mesh):
    in_specs = (P(AX, None), P(None, AX))
    return jax.shard_map(reduce_all, mesh=mesh, in_specs=in_specs, out_specs=P(AX, None), check_vma=False)
```

```python
import functools

import jax
import jax.numpy as jnp
from jax import lax
from jax.experimental import pallas as pl
from jax.experimental.pallas import tpu as pltpu
from jax.sharding import PartitionSpec as P

WINDOW = 256
LANE = 128
TILE = WINDOW + 8
AX = ("rows", "grp")
FLIP = (1, 3)
PARTS = ((4, 5, 1), (2, 3, 0), (6, 7))
ORDER = ((0, 1, 2), (1, 2, 0), (2, 0, 1))
COUNT = tuple(4 * len(p) for p in PARTS)
START = (0, COUNT[0], COUNT[0] + COUNT[1])
TOTAL = sum(COUNT)
SIDE = tuple(((0, j), (1, j)) for j in range(4))
PAIRS = (
    SIDE + (((2, 0), (2, 1)), ((2, 2), (2, 3))),
    SIDE + (((2, 0), (2, 2)), ((2, 1), (2, 3))),
    SIDE,
)
QUEUE = (2, 0, 1)


def linear(x, y, z, c):
    return ((y * 2 + (x >> 1)) * 2 + c) * 8 + (x & 1) * 4 + z


def place(i):
    r, g = i >> 3, i & 7
    return (((r >> 1) & 1) * 2 + (g >> 2), r >> 2, g & 3, r & 1)


def swap_cores():
    return [(i, i ^ 8) for i in range(128)]


def flips(bits, phase):
    out = []
    for i in range(128):
        k = list(place(i))
        by = FLIP[k[3] ^ phase]
        for d in range(3):
            if bits[d]:
                k[d] ^= by
        out.append((i, linear(*k)))
    return out


def bits_of(s):
    return (s >> 2 & 1, s >> 1 & 1, s & 1)


def f_bits(part, half, j):
    f = [0, 0, 0]
    for d, b in zip(ORDER[part], (half, j >> 1, j & 1)):
        f[d] = b
    return f


def gram_kernel(own, half, first, here, matrix, mask, *refs):
    if first:
        *outs, panel_t, stat, gates, tiles, sems, panel, flags, panel_sems = refs
    else:
        gates = mask
        panel_t, stat, *rest = refs
        *outs, tiles, sems = rest[-5:]
    x, y, z, c = place(here[0])
    c = c if own else 1 - c
    near, far = 1 + 2 * c, 3 - 2 * c

    def goal(part, n, j):
        f, s = f_bits(part, half, j), bits_of(PARTS[part][n])
        by = [(0, far, near, 2)[2 * fb + sb] for fb, sb in zip(f, s)]
        return linear(x ^ by[0], y ^ by[1], z ^ by[2], c)

    def fetch(t, at):
        return pltpu.make_async_copy(matrix.at[:, pl.ds(at * LANE, LANE)], tiles.at[t], sems.at[t])

    if first:
        whole = pltpu.make_async_copy(matrix.at[:, pl.ds(0, WINDOW)], panel, panel_sems.at[0])
        whole.start()
        masks = pltpu.make_async_copy(mask, flags, panel_sems.at[1])
        masks.start()
    for p in range(3):
        for pair in PAIRS[p]:
            for n, j in pair:
                fetch(START[p] + 4 * n + j, goal(p, n, j)).start()
    if first:
        masks.wait()
        gates[...] = (flags[...] * flags[0:1, :]).astype(jnp.float32)
        whole.wait()
        panel_t[...] = panel[...].T
        q = jnp.sum(jnp.square(panel[...].astype(jnp.float32)), axis=0, keepdims=True)
        stat[...] = jnp.concatenate([jnp.zeros((1, LANE), jnp.float32), q[:, :LANE], q[:, LANE:], jnp.zeros((5, LANE), jnp.float32)], axis=0)
    top_row = lax.broadcasted_iota(jnp.int32, (8, LANE), 0) == 0

    for p in range(3):
        for t in range(COUNT[p]):
            fetch(START[p] + t, 0).wait()
        for pair in PAIRS[p]:
            gate = gates[pl.ds(goal(p, *pair[0]) // 8, 1), :].astype(jnp.bfloat16)
            both = jnp.concatenate([tiles[START[p] + 4 * n + j] for n, j in pair], axis=1)
            acc = jnp.dot(panel_t[...] * gate, both, preferred_element_type=jnp.float32)
            square = jnp.sum(jnp.square(both.astype(jnp.float32)), axis=0, keepdims=True)
            for k, (n, j) in enumerate(pair):
                cut = slice(k * LANE, (k + 1) * LANE)
                out, at = outs[p], j * len(PARTS[p]) + n
                out[at, :WINDOW] = acc[:, cut]
                out[at, WINDOW:] = jnp.where(top_row, square[:, cut], stat[...])


def gram(own, half, here, matrix, mask, extra=()):
    rows = matrix.shape[0]
    first = not extra
    vmem = pl.BlockSpec(memory_space=pltpu.VMEM)
    hbm = pl.BlockSpec(memory_space=pltpu.HBM)
    shapes = [jax.ShapeDtypeStruct((n, TILE, LANE), jnp.float32) for n in COUNT]
    scratch = [pltpu.VMEM((TOTAL, rows, LANE), jnp.bfloat16), pltpu.SemaphoreType.DMA((TOTAL,))]
    if first:
        shapes += [jax.ShapeDtypeStruct((WINDOW, rows), jnp.bfloat16), jax.ShapeDtypeStruct((8, LANE), jnp.float32), jax.ShapeDtypeStruct(mask.shape, jnp.float32)]
        scratch += [pltpu.VMEM((rows, WINDOW), jnp.bfloat16), pltpu.VMEM(mask.shape, jnp.int32), pltpu.SemaphoreType.DMA((2,))]
    return pl.pallas_call(
        functools.partial(gram_kernel, own, half, first),
        out_shape=tuple(shapes),
        in_specs=[pl.BlockSpec(memory_space=pltpu.SMEM), hbm]
        + ([hbm] if first else [vmem] * 3 + [pl.BlockSpec(memory_space=pl.ANY)] * (len(extra) - 2)),
        out_specs=tuple(vmem for _ in shapes),
        scratch_shapes=scratch,
        compiler_params=pltpu.CompilerParams(vmem_limit_bytes=20 << 20),
        cost_estimate=pl.CostEstimate(
            flops=2 * rows * WINDOW * LANE * TOTAL, bytes_accessed=rows * LANE * 2 * TOTAL, transcendentals=0
        ),
    )(here, matrix, mask, *extra)


def finish_kernel(own, a, b, c, d, out):
    total = own[0] + a[0] + b[0] + c[0] + d[0]
    inverse = 1.0 / jnp.sqrt(total[WINDOW:] + 1e-06)
    scaled = total[:WINDOW] * inverse[0:1]
    for h in range(WINDOW // LANE):
        out[:, h * LANE : (h + 1) * LANE] = scaled[h * LANE : (h + 1) * LANE].T * inverse[1 + h : 2 + h]


def send(value, pairs):
    return lax.ppermute(value, AX, pairs)


def total_kernel(starts, size, *refs):
    value = refs[0][pl.ds(starts[0], size)]
    for r, at in zip(refs[1:-1], starts[1:]):
        value = value + r[pl.ds(at, size)]
    refs[-1][...] = value


def total(values, starts, size):
    vmem = pl.BlockSpec(memory_space=pltpu.VMEM)
    return pl.pallas_call(
        functools.partial(total_kernel, starts, size),
        out_shape=jax.ShapeDtypeStruct((size, TILE, LANE), jnp.float32),
        in_specs=[vmem] * len(values),
        out_specs=vmem,
        compiler_params=pltpu.CompilerParams(vmem_limit_bytes=4 << 20),
    )(*values)


def follow(value, *others):
    return lax.optimization_barrier((value, *others))[0]


def reduce_all(matrix, keep_mask):
    here = (lax.axis_index("rows") * 8 + lax.axis_index("grp")).astype(jnp.int32).reshape(1)
    unit = lambda d: tuple(int(d == k) for k in range(3))
    matrix = pltpu.with_memory_space_constraint(matrix, pltpu.HBM)
    *peer, panel_t, stat, gates = gram(0, 1, here, matrix, pltpu.with_memory_space_constraint(keep_mask, pltpu.HBM))
    got = [send(a, swap_cores()) for a in peer]
    own = gram(1, 1, here, matrix, gates, (panel_t, stat, *peer))
    first = [own[0] + got[0]]
    for p in (1, 2):
        first.append(own[p] + follow(got[p], first[-1]))
    r1 = [send(first[p], flips(unit(ORDER[p][0]), 0)) for p in range(3)]
    peer = gram(0, 0, here, matrix, gates, (panel_t, stat, *first))
    got = [send(a, swap_cores()) for a in peer]
    own = gram(1, 0, here, matrix, gates, (panel_t, stat, *peer))

    r2, r3, o1 = [None] * 3, [None] * 3, [None] * 3
    rest = [None] * 3
    last = first[2]
    for p in QUEUE:
        n = len(PARTS[p])
        got[p] = follow(got[p], last)
        last = own[p][2 * n :] + got[p][2 * n :] + r1[p][2 * n :]
        r2[p] = send(last, flips(unit(ORDER[p][1]), 0))
        rest[p] = total((own[p], got[p], r1[p]), (0, 0, 0), 2 * n)
    for p in QUEUE:
        n = len(PARTS[p])
        last = rest[p][n:] + follow(r2[p], last)[n:]
        r3[p] = send(last, flips(unit(ORDER[p][2]), 0))
        rest[p] = total((rest[p], r2[p]), (0, 0), n)
    for p in QUEUE:
        last = rest[p][:2] + follow(r3[p], last)[:2]
        o1[p] = send(last, flips(((1, 0, 0), (0, 1, 0), (1, 1, 0))[p], 1))
    left = [total((rest[p], r3[p]), (2, 2), 1) for p in (0, 1)]
    o2 = send(left[0] + o1[0][1:] + o1[1][1:] + o1[2][1:], flips((0, 0, 1), 1))
    return pl.pallas_call(
        finish_kernel,
        out_shape=jax.ShapeDtypeStruct((LANE, WINDOW), jnp.float32),
        name="finish",
        compiler_params=pltpu.CompilerParams(vmem_limit_bytes=8 << 20),
    )(left[1], *o1, o2)


def solution(mesh):
    in_specs = (P(AX, None), P(None, AX))
    return jax.shard_map(reduce_all, mesh=mesh, in_specs=in_specs, out_specs=P(AX, None), check_vma=False)
```
